8 devices in a mesh: mp: 1 (over z), dpa: 2 (over y), dpb: 2 (over x), dpc: 2 (over core).
Axes of the slice: x: 2, y: 2, z: 1, core: 2. Of those that a mesh axis runs over, the one named last changes fastest.
Arguments:
- x: bfloat16 [8192, 2048], P(('mp', 'dpa', 'dpb', 'dpc'))
- g: bfloat16 [8192, 2048], P(('mp', 'dpa', 'dpb', 'dpc'))
- w1: bfloat16 [2048, 8192], P('mp')
- w2: bfloat16 [8192, 2048], P('mp')
- w3: bfloat16 [2048, 8192], P('mp')
- w4: bfloat16 [8192, 2048], P('mp')
Outputs:
- output 1: float32 [2048, 8192], P('mp')
- output 2: float32 [8192, 2048], P('mp')
- output 3: float32 [2048, 8192], P('mp')
- output 4: float32 [8192, 2048], P('mp')
- output 5: bfloat16 [8192, 2048], P(('mp', 'dpa', 'dpb', 'dpc'))
All inputs are finite; a program needn't handle non-finite values.
Results may differ from the reference program's by a relative error of at most 0.0114265.
Values are sent between devices in bfloat16 or wider.
A program may use at most 1.75 GiB of HBM per device.

```python
import jax
import jax.numpy as jnp
from jax import lax

D = 2048
F = 8192
TOKENS_DEV = 1024
NDEV = 8
B = TOKENS_DEV * NDEV


def setup_inputs(seed: int = 0, part: int = 0) -> dict:
    key = jax.random.fold_in(jax.random.key(seed), part)
    ks = jax.random.split(key, 6)
    x = jax.random.normal(ks[0], (B, D), jnp.float32)
    g = jax.random.normal(ks[1], (B, D), jnp.float32)
    w1 = jax.random.normal(ks[2], (D, F), jnp.float32) * D ** -0.5
    w2 = jax.random.normal(ks[3], (F, D), jnp.float32) * F ** -0.5
    w3 = jax.random.normal(ks[4], (D, F), jnp.float32) * D ** -0.5
    w4 = jax.random.normal(ks[5], (F, D), jnp.float32) * F ** -0.5
    return {"x": x.astype(jnp.bfloat16), "g": g.astype(jnp.bfloat16), "w1": w1.astype(jnp.bfloat16), "w2": w2.astype(jnp.bfloat16), "w3": w3.astype(jnp.bfloat16), "w4": w4.astype(jnp.bfloat16)}


def gelu_grad(a, d):
    return jax.vjp(lambda t: jax.nn.gelu(t, approximate=True), a)[1](d)[0]


def block_grads(x, g, w1, w2, w3, w4):
    f32 = jnp.float32
    bf = jnp.bfloat16
    a1 = jnp.dot(x, w1, preferred_element_type=f32).astype(bf)
    h1 = jax.nn.gelu(a1.astype(f32), approximate=True).astype(bf)
    h2 = (jnp.dot(h1, w2, preferred_element_type=f32) + x.astype(f32)).astype(bf)
    a3 = jnp.dot(h2, w3, preferred_element_type=f32).astype(bf)
    h3 = jax.nn.gelu(a3.astype(f32), approximate=True).astype(bf)
    dw4 = jnp.dot(h3.T, g, preferred_element_type=f32)
    dh3 = jnp.dot(g, w4.T, preferred_element_type=f32).astype(bf)
    da3 = gelu_grad(a3.astype(f32), dh3.astype(f32)).astype(bf)
    dw3 = jnp.dot(h2.T, da3, preferred_element_type=f32)
    dh2 = (jnp.dot(da3, w3.T, preferred_element_type=f32) + g.astype(f32)).astype(bf)
    dw2 = jnp.dot(h1.T, dh2, preferred_element_type=f32)
    dh1 = jnp.dot(dh2, w2.T, preferred_element_type=f32).astype(bf)
    da1 = gelu_grad(a1.astype(f32), dh1.astype(f32)).astype(bf)
    dw1 = jnp.dot(x.T, da1, preferred_element_type=f32)
    dx = (jnp.dot(da1, w1.T, preferred_element_type=f32) + dh2.astype(f32)).astype(bf)
    return dw1, dw2, dw3, dw4, dx


def reference(x, g, w1, w2, w3, w4):
    xs = x.reshape(NDEV, TOKENS_DEV, D)
    gs = g.reshape(NDEV, TOKENS_DEV, D)

    def body(acc, xg):
        res = block_grads(xg[0], xg[1], w1, w2, w3, w4)
        acc = tuple(a + b for a, b in zip(acc, res[:4]))
        return acc, res[4]

    zero = (jnp.zeros((D, F), jnp.float32), jnp.zeros((F, D), jnp.float32), jnp.zeros((D, F), jnp.float32), jnp.zeros((F, D), jnp.float32))
    acc, dxs = lax.scan(body, zero, (xs, gs))
    return acc[0] / NDEV, acc[1] / NDEV, acc[2] / NDEV, acc[3] / NDEV, dxs.reshape(B, D)
```

```python
import jax
import jax.numpy as jnp
from jax import lax
from jax.sharding import PartitionSpec as P


GROUP = ("dpa", "dpb", "dpc")
f32 = jnp.float32
bf = jnp.bfloat16


def gelu(a):
    return jax.nn.gelu(a.astype(f32), approximate=True).astype(bf)


def gelu_grad(a, d):
    return jax.vjp(lambda t: jax.nn.gelu(t, approximate=True), a.astype(f32))[1](d.astype(f32))[0].astype(bf)


def nn(a, b):
    return jnp.dot(a, b, preferred_element_type=f32)


def nt(a, b):
    return lax.dot_general(a, b, (((1,), (1,)), ((), ())), preferred_element_type=f32)


def tn(a, b):
    return lax.dot_general(a, b, (((0,), (0,)), ((), ())), preferred_element_type=f32)


def solution(mesh):
    ndev = mesh.shape["dpa"] * mesh.shape["dpb"] * mesh.shape["dpc"]
    ncore = mesh.shape["dpc"]
    rows = P(("mp",) + GROUP, None)
    wspec = P("mp", None)

    def swap(v):
        return lax.ppermute(v, "dpc", [(i, ncore - 1 - i) for i in range(ncore)])

    def join(mine, theirs, axis):
        core = lax.axis_index("dpc")
        n = mine.shape[axis]
        shape = list(mine.shape)
        shape[axis] = 2 * n
        out = jnp.zeros(shape, mine.dtype)
        out = lax.dynamic_update_slice_in_dim(out, mine, core * n, axis)
        return lax.dynamic_update_slice_in_dim(out, theirs, (1 - core) * n, axis)

    def after(v, *deps):
        return lax.optimization_barrier((v,) + deps)[0]

    def gather(v):
        return lax.all_gather(v, GROUP, axis=0, tiled=True)

    def local(x, g, w1, w2, w3, w4):
        ff = w1.shape[1]
        gs = gather(g)
        a1 = nn(x, w1).astype(bf)
        h2 = (nn(gelu(a1), w2) + x.astype(f32)).astype(bf)
        h2s = gather(h2)
        a3 = nn(h2, w3).astype(bf)
        xs = gather(after(x, a3))
        da3 = gelu_grad(a3, nt(g, w4).astype(bf))
        dh2 = (nt(da3, w3) + g.astype(f32)).astype(bf)
        dh2s = gather(dh2)
        da1 = gelu_grad(a1, nt(dh2, w2).astype(bf))
        dx = (nt(da1, w1) + dh2.astype(f32)).astype(bf)

        n34 = ff // ndev
        i34 = lax.axis_index(GROUP) * n34
        w3c = lax.dynamic_slice_in_dim(w3, i34, n34, axis=1)
        w4c = lax.dynamic_slice_in_dim(w4, i34, n34, axis=0)
        h2s = after(h2s, dx)
        a3c = nn(h2s, w3c).astype(bf)
        dw4c = tn(gelu(a3c), gs)
        dw4s = gather(dw4c)
        da3c = gelu_grad(a3c, nt(after(gs, dw4c), w4c).astype(bf))
        dw3c = tn(h2s, da3c) / ndev
        dw3s = lax.all_gather(dw3c, GROUP, axis=0, tiled=False)

        n12 = ff // ncore
        i12 = lax.axis_index("dpc") * n12
        w1c = lax.dynamic_slice_in_dim(w1, i12, n12, axis=1)
        w2c = lax.dynamic_slice_in_dim(w2, i12, n12, axis=0)
        xs = after(xs, dw3c)
        a1c = nn(xs, w1c).astype(bf)
        dw2c = tn(gelu(a1c), dh2s) / ndev
        dw2o = swap(dw2c)
        da1c = gelu_grad(a1c, nt(after(dh2s, dw2c), w2c).astype(bf))
        dw2 = join(dw2c, after(dw2o, da1c), 0)
        da1c, dw4s = lax.optimization_barrier((da1c, dw4s))
        dw4 = dw4s / ndev
        dw1c = tn(xs, after(da1c, dw2, dw4)) / ndev
        dw1o = swap(dw1c)
        dw1 = join(dw1c, dw1o, 1)
        dw3 = jnp.swapaxes(after(dw3s, dw1c), 0, 1).reshape(dw3s.shape[1], ff)
        return dw1, dw2, dw3, dw4, dx

    return jax.shard_map(local, mesh=mesh, in_specs=(rows, rows, wspec, wspec, wspec, wspec), out_specs=(wspec, wspec, wspec, wspec, rows), check_vma=False)
```

```python
import functools
import math

import jax
import jax.numpy as jnp
from jax import lax
from jax.experimental import pallas as pl
from jax.experimental.pallas import tpu as pltpu
from jax.sharding import PartitionSpec as P


GROUP = ("dpa", "dpb", "dpc")
f32 = jnp.float32
bf = jnp.bfloat16


def gelu(a):
    return jax.nn.gelu(a.astype(f32), approximate=True).astype(bf)


C0 = (2.0 / math.pi) ** 0.5
C1 = 0.044715 * C0


def grad_kernel(sub, off_ref, d_ref, w_ref, a_ref, o_ref):
    for i in range(d_ref.shape[0] // sub):
        at = pl.ds(i * sub, sub)
        y = nt(d_ref[at, :], w_ref[...]).astype(bf).astype(f32)
        a = a_ref[at, :].astype(f32)
        sq = a * a
        t = jnp.tanh(a * (C0 + C1 * sq))
        h = 0.5 + 0.5 * t
        slope = h + ((h * (1.0 - t)) * a) * (C0 + 3.0 * C1 * sq)
        o_ref[at, :] = (y * slope).astype(bf)


def nt_gelu_grad(d, w, a, first=None, bm=2048, bn=512, sub=512):
    m, k = d.shape
    n = a.shape[1]
    if m < bm:
        bm, bn = m, bm * bn // m
    off = jnp.zeros((1,), jnp.int32) if first is None else (first // bn).astype(jnp.int32).reshape(1)
    return pl.pallas_call(
        functools.partial(grad_kernel, sub),
        out_shape=jax.ShapeDtypeStruct((m, n), bf),
        grid_spec=pltpu.PrefetchScalarGridSpec(
            num_scalar_prefetch=1,
            grid=(m // bm, n // bn),
            in_specs=[
                pl.BlockSpec((bm, k), lambda i, j, o: (i, 0)),
                pl.BlockSpec((bn, k), lambda i, j, o: (j + o[0], 0)),
                pl.BlockSpec((bm, bn), lambda i, j, o: (i, j)),
            ],
            out_specs=pl.BlockSpec((bm, bn), lambda i, j, o: (i, j)),
        ),
        cost_estimate=pl.CostEstimate(flops=2 * m * n * k, bytes_accessed=2 * (m * k + n * k + 2 * m * n), transcendentals=m * n),
        name="nt_gelu_grad",
    )(off, d, w, a)


def place_kernel(p_ref, full_ref, o_ref):
    o_ref[...] = p_ref[...]


def place(full, parts, row, rows=256):
    n, m, width = parts.shape
    return pl.pallas_call(
        place_kernel,
        out_shape=jax.ShapeDtypeStruct(full.shape, full.dtype),
        grid=(m // rows, n),
        in_specs=[pl.BlockSpec((None, rows, width), lambda i, d: (d, i, 0)), pl.BlockSpec(memory_space=pl.ANY)],
        out_specs=pl.BlockSpec((rows, width), lambda i, d: (row // rows + i, d)),
        input_output_aliases={1: 0},
        cost_estimate=pl.CostEstimate(flops=n * m * width, bytes_accessed=8 * n * m * width, transcendentals=0),
        name="place",
    )(parts, full)


def empty(shape, dtype):
    return pl.pallas_call(
        lambda o_ref: None,
        out_shape=jax.ShapeDtypeStruct(shape, dtype),
        out_specs=pl.BlockSpec(memory_space=pl.ANY),
        name="empty",
    )()


def nn(a, b):
    return jnp.dot(a, b, preferred_element_type=f32)


def nt(a, b):
    return lax.dot_general(a, b, (((1,), (1,)), ((), ())), preferred_element_type=f32)


def tn(a, b):
    return lax.dot_general(a, b, (((0,), (0,)), ((), ())), preferred_element_type=f32)


def solution(mesh):
    ndev = mesh.shape["dpa"] * mesh.shape["dpb"] * mesh.shape["dpc"]
    ncore = mesh.shape["dpc"]
    rows = P(("mp",) + GROUP, None)
    wspec = P("mp", None)

    def swap(v):
        return lax.ppermute(v, "dpc", [(i, ncore - 1 - i) for i in range(ncore)])

    def join(mine, theirs, axis):
        core = lax.axis_index("dpc")
        n = mine.shape[axis]
        shape = list(mine.shape)
        shape[axis] = 2 * n
        out = empty(shape, mine.dtype)
        out = lax.dynamic_update_slice_in_dim(out, mine, core * n, axis)
        return lax.dynamic_update_slice_in_dim(out, theirs, (1 - core) * n, axis)

    def after(v, *deps):
        return lax.optimization_barrier((v,) + deps)[0]

    def gather(v, tiled=True):
        return lax.all_gather(v, GROUP, axis=0, tiled=tiled)

    def local(x, g, w1, w2, w3, w4):
        ff = w1.shape[1]
        gs = gather(g)
        a1 = nn(x, w1).astype(bf)
        h2 = (nn(gelu(a1), w2) + x.astype(f32)).astype(bf)
        h2s = gather(h2)
        a3 = nn(h2, w3).astype(bf)
        xs = gather(after(x, a3))
        da3 = nt_gelu_grad(g, w4, a3)
        dh2 = (nt(da3, w3) + g.astype(f32)).astype(bf)
        dh2s = gather(dh2)
        da1 = nt_gelu_grad(dh2, w2, a1)
        dx = (nt(da1, w1) + dh2.astype(f32)).astype(bf)

        n34 = ff // ndev
        i34 = lax.axis_index(GROUP) * n34
        w3c = lax.dynamic_slice_in_dim(w3, i34, n34, axis=1)
        h2s = after(h2s, dx)
        a3c = nn(h2s, w3c).astype(bf)
        dw4c = tn(gelu(a3c), gs)
        dw4s = gather(dw4c)
        da3c = nt_gelu_grad(after(gs, dw4c), w4, a3c, i34)
        dw3c = tn(h2s, da3c) / ndev
        half = dw3c.shape[0] // 2
        dw3s = [gather(dw3c[i * half : (i + 1) * half], False) for i in range(2)]

        n12 = ff // ncore
        i12 = lax.axis_index("dpc") * n12
        w1c = lax.dynamic_slice_in_dim(w1, i12, n12, axis=1)
        xs = after(xs, dw3c)
        a1c = nn(xs, w1c).astype(bf)
        dw2c = tn(gelu(a1c), dh2s) / ndev
        dw2o = swap(dw2c)
        da1c = nt_gelu_grad(after(dh2s, dw2c), w2, a1c, i12)
        dw2 = join(dw2c, after(dw2o, da1c), 0)
        da1c, dw4s = lax.optimization_barrier((da1c, dw4s))
        dw4 = dw4s / ndev
        dw1c = tn(xs, after(da1c, dw2, dw4)) / ndev
        dw1o = swap(dw1c)
        dw3 = empty((dw3c.shape[0], ff), f32)
        for i in range(2):
            dw3 = place(dw3, after(dw3s[i], dw1c, dw3), i * half)
        dw1 = join(dw1c, dw1o, 1)
        return dw1, dw2, dw3, dw4, dx

    return jax.shard_map(local, mesh=mesh, in_specs=(rows, rows, wspec, wspec, wspec, wspec), out_specs=(wspec, wspec, wspec, wspec, rows), check_vma=False)
```
